32 devices in a mesh: gx: 16 (over z, y, x), gz: 2 (over core).
Axes of the slice: x: 2, y: 2, z: 4, core: 2. Of those that a mesh axis runs over, the one named last changes fastest.
Arguments:
- state: float32 [5, 128, 16, 256], P(None, 'gx', None, 'gz'), may hold values from -1 to 8.5, as said below
- register: float32 [5, 128, 16, 256], P(None, 'gx', None, 'gz'), may hold values from -2.4 to 2.4
- top_ghost: float32 [5, 128, 3, 256], P(None, 'gx', None, 'gz'), may hold values from -1 to 8.5, as said below
- flags: int32 [128, 16, 2], P('gx', None, 'gz'), may hold values 0 or 1
Outputs:
- new_state: float32 [5, 128, 16, 256], P(None, 'gx', None, 'gz')
- new_register: float32 [5, 128, 16, 256], P(None, 'gx', None, 'gz')
The draws below stay inside these ranges and needn't reach their ends.
Inputs may be any that keep to these rules, and one draw needn't show every extreme that they name: `state`: conserved variables of an ideal gas with ratio of heats 1.4, density 0.5 to 2 and pressure 0.3 to 1.5 in every cell. `top_ghost`: conserved variables of an ideal gas with ratio of heats 1.4, density 0.5 to 2 and pressure 0.3 to 1.5 in every cell.
All inputs are finite; a program needn't handle non-finite values. No bound on the sum of `flags` on one device may be relied on, other than what follows from the above.
Results may differ from the reference program's by a relative error of at most 0.0003.
Values sent between devices are 32-bit elements; how exact they have to be, the bound alone decides.
A program may use at most 64 MiB of HBM per device.

```python
import math
import jax
import jax.numpy as jnp
from jax import lax

CX = 8
NY = 16
CZ = 128
ZBLOCK = 128
NX = 128
NZ = 256
N_GX = 16


def speed_levels(key):
    keys = jax.random.split(jax.random.fold_in(key, 31), 2)
    stream_count = NX // CX
    span_count = NZ // CZ
    base = jax.random.uniform(keys[0], (stream_count,), jnp.float32, 0.0, 1.0)
    stream_level = 0.6 + 0.4 * base * base * base * base
    span_level = jax.random.uniform(keys[1], (span_count,), jnp.float32, 0.6, 1.0)
    stream_cells = jnp.repeat(stream_level, CX, total_repeat_length=NX)
    span_cells = jnp.repeat(span_level, CZ, total_repeat_length=NZ)
    return stream_cells[:, None, None] * span_cells[None, None, :]


def gas_state(key, shape, level):
    keys = jax.random.split(key, 5)
    density = jnp.exp(jax.random.uniform(keys[0], shape, jnp.float32, math.log(0.5), math.log(2.0)))
    vel_x = jax.random.uniform(keys[1], shape, jnp.float32, 0.4, 2.0)
    vel_y = jax.random.uniform(keys[2], shape, jnp.float32, -0.5, 0.5)
    vel_z = jax.random.uniform(keys[3], shape, jnp.float32, -0.5, 0.5)
    pressure = jnp.exp(jax.random.uniform(keys[4], shape, jnp.float32, math.log(0.3), math.log(1.5)))
    vel_x = vel_x * level
    vel_y = vel_y * level
    vel_z = vel_z * level
    energy = pressure / 0.4 + 0.5 * density * (vel_x * vel_x + vel_y * vel_y + vel_z * vel_z)
    return jnp.stack([density, density * vel_x, density * vel_y, density * vel_z, energy])


def draw_state(key, part):
    return gas_state(jax.random.fold_in(key, 11), (NX, NY, NZ), speed_levels(key))


def draw_top_ghost(key, part):
    return gas_state(jax.random.fold_in(key, 23), (NX, 3, NZ), speed_levels(key))


def set_ends(result, key, low, largest):
    shape = result.shape
    spot = [jax.random.randint(jax.random.fold_in(key, axis), (), 0, shape[axis]) for axis in range(len(shape))]
    result = result.at[tuple(spot)].set(low)
    longest = shape.index(max(shape))
    spot[longest] = (spot[longest] + 1) % shape[longest]
    return result.at[tuple(spot)].set(largest)


def level_of(stream_key, dims, cuts, smallest, top_value):
    loudness, own = 1.0, jax.random.fold_in(stream_key, 6)
    for dim, blocks in cuts:
        heights = jnp.exp(jax.random.uniform(jax.random.fold_in(own, dim), (blocks,), jnp.float32, smallest / len(cuts), top_value / len(cuts)))
        loudness = loudness * jnp.repeat(heights, dims[dim] // blocks).reshape([-1 if axis == dim else 1 for axis in range(len(dims))])
    return loudness


def normal_values(key, extent, spread, reach, cuts=(), kind=jnp.bfloat16):
    factor_of = level_of(key, extent, cuts, -0.22, 0.18) if cuts else 1.0
    result = jax.random.normal(key, extent, jnp.float32) * spread * factor_of
    return jnp.minimum(jnp.maximum(result, -reach), reach).astype(kind)


def setup_inputs(seed: int = 0) -> dict:
    streams_of = jax.random.split(jax.random.key(seed), 5)
    return {
        "state": draw_state(jax.random.fold_in(streams_of[4], 71), 0),
        "register": normal_values(streams_of[1], (5, NX, NY, NZ), 0.4, 2.4, ((1, 16), (3, 2)), jnp.float32),
        "top_ghost": draw_top_ghost(jax.random.fold_in(streams_of[4], 71), 0),
        "flags": set_ends((jax.random.randint(streams_of[3], (NX, NY, NZ // ZBLOCK), 0, 2) < 1).astype(jnp.int32), jax.random.fold_in(streams_of[3], 1), 0, 1),
    }


GAMMA = 1.4
EPS_WENO = 1e-06
LAMBDA_X = 0.1
LAMBDA_Y = 0.15
LAMBDA_Z = 0.1
REGISTER_DECAY = -5.0 / 9.0
UPDATE_WEIGHT = 15.0 / 16.0

def primitives(cons):
    density = cons[0]
    inverse = 1.0 / density
    vel_x = cons[1] * inverse
    vel_y = cons[2] * inverse
    vel_z = cons[3] * inverse
    pressure = (GAMMA - 1.0) * (cons[4] - 0.5 * (cons[1] * vel_x + cons[2] * vel_y + cons[3] * vel_z))
    return (density, vel_x, vel_y, vel_z, pressure)

def local_speeds(prims):
    density, vel_x, vel_y, vel_z, pressure = prims
    sound = jnp.sqrt(GAMMA * pressure / density)
    return jnp.stack([jnp.max(jnp.abs(vel_x) + sound), jnp.max(jnp.abs(vel_y) + sound), jnp.max(jnp.abs(vel_z) + sound)])

def physical_flux(cons, prims, var):
    pressure = prims[4]
    velocity = prims[var]
    rows = [cons[0] * velocity, cons[1] * velocity, cons[2] * velocity, cons[3] * velocity, (cons[4] + pressure) * velocity]
    rows[var] = rows[var] + pressure
    return jnp.stack(rows)

def weno_face(vals):
    first, second, third, fourth, fifth = vals
    cand_a = (2.0 * first - 7.0 * second + 11.0 * third) / 6.0
    cand_b = (-second + 5.0 * third + 2.0 * fourth) / 6.0
    cand_c = (2.0 * third + 5.0 * fourth - fifth) / 6.0
    smooth_a = 13.0 / 12.0 * (first - 2.0 * second + third) ** 2 + 0.25 * (first - 4.0 * second + 3.0 * third) ** 2
    smooth_b = 13.0 / 12.0 * (second - 2.0 * third + fourth) ** 2 + 0.25 * (second - fourth) ** 2
    smooth_c = 13.0 / 12.0 * (third - 2.0 * fourth + fifth) ** 2 + 0.25 * (3.0 * third - 4.0 * fourth + fifth) ** 2
    weight_a = 0.1 / (EPS_WENO + smooth_a) ** 2
    weight_b = 0.6 / (EPS_WENO + smooth_b) ** 2
    weight_c = 0.3 / (EPS_WENO + smooth_c) ** 2
    return (weight_a * cand_a + weight_b * cand_b + weight_c * cand_c) / (weight_a + weight_b + weight_c)

def divergence(padded, prims, alpha, var, axis_pos, count, cell_flag):
    flux = physical_flux(padded, prims, var)
    plus = 0.5 * (flux + alpha * padded)
    minus = 0.5 * (flux - alpha * padded)

    def window(arr, offset):
        return lax.slice_in_dim(arr, offset, offset + count + 1, axis=axis_pos)
    central = (37.0 * (window(flux, 2) + window(flux, 3)) - 8.0 * (window(flux, 1) + window(flux, 4)) + (window(flux, 0) + window(flux, 5))) / 60.0
    upwind = weno_face([window(plus, 0), window(plus, 1), window(plus, 2), window(plus, 3), window(plus, 4)])
    upwind = upwind + weno_face([window(minus, 5), window(minus, 4), window(minus, 3), window(minus, 2), window(minus, 1)])

    def jump(face):
        return lax.slice_in_dim(face, 1, count + 1, axis=axis_pos) - lax.slice_in_dim(face, 0, count, axis=axis_pos)
    return jnp.where(cell_flag[None], jump(upwind), jump(central))

def wall_pad(inner, top_ghost):
    mirror = jnp.array([1.0, 1.0, -1.0, 1.0, 1.0], dtype=jnp.float32).reshape(5, 1, 1, 1)
    lower = jnp.flip(inner[:, :, :3], axis=2) * mirror
    return jnp.concatenate([lower, inner, top_ghost], axis=2)

def expand_flags(flags):
    shape = flags.shape
    wide = jnp.broadcast_to(flags[:, :, :, None], (shape[0], shape[1], shape[2], ZBLOCK))
    return wide.reshape(shape[0], shape[1], shape[2] * ZBLOCK) > 0

def advance(inner, x_pad, z_pad, y_pad, register, cell_flag, alpha, x_prims):
    div_x = divergence(x_pad, x_prims, alpha[0], 1, 1, inner.shape[1], cell_flag)
    div_y = divergence(y_pad, primitives(y_pad), alpha[1], 2, 2, inner.shape[2], cell_flag)
    div_z = divergence(z_pad, primitives(z_pad), alpha[2], 3, 3, inner.shape[3], cell_flag)
    change = -(LAMBDA_X * div_x + LAMBDA_Y * div_y + LAMBDA_Z * div_z)
    new_register = REGISTER_DECAY * register + change
    new_state = inner + UPDATE_WEIGHT * new_register
    return (new_state, new_register)

def reference(state, register, top_ghost, flags):
    blocks = jnp.arange(N_GX, dtype=jnp.int32)

    def block_speeds(index):
        inner = lax.dynamic_slice_in_dim(state, index * CX, CX, 1)
        return local_speeds(primitives(inner))
    alpha = lax.optimization_barrier(jnp.max(lax.map(block_speeds, blocks), axis=0))

    def block_update(index):
        start = index * CX
        rows = (start - 3 + jnp.arange(CX + 6, dtype=jnp.int32)) % NX
        x_pad = jnp.take(state, rows.astype(jnp.int32), axis=1)
        inner = lax.dynamic_slice_in_dim(state, start, CX, 1)
        reg_block = lax.dynamic_slice_in_dim(register, start, CX, 1)
        top_block = lax.dynamic_slice_in_dim(top_ghost, start, CX, 1)
        flag_block = lax.dynamic_slice_in_dim(flags, start, CX, 0)
        z_pad = jnp.concatenate([inner[:, :, :, NZ - 3:], inner, inner[:, :, :, :3]], axis=3)
        y_pad = wall_pad(inner, top_block)
        return advance(inner, x_pad, z_pad, y_pad, reg_block, expand_flags(flag_block), alpha, primitives(x_pad))
    states, registers = lax.map(block_update, blocks)
    new_state = jnp.moveaxis(states, 0, 1).reshape(5, NX, NY, NZ)
    new_register = jnp.moveaxis(registers, 0, 1).reshape(5, NX, NY, NZ)
    return (new_state, new_register)
```

```python
import functools

import jax
import jax.numpy as jnp
from jax import lax
from jax.experimental import pallas as pl
from jax.experimental.pallas import tpu as pltpu
from jax.sharding import PartitionSpec as P

MESH = pl.DeviceIdType.MESH
GAMMA = 1.4
EPS_WENO = 1e-06
LAMBDA = (0.1, 0.15, 0.1)
REGISTER_DECAY = -5.0 / 9.0
UPDATE_WEIGHT = 15.0 / 16.0
UNROLL_LIMIT = 64


def reciprocal(value):
    guess = pl.reciprocal(value, approx=True)
    return guess * (2.0 - value * guess)


def pressure_velocity(cons):
    inverse = reciprocal(cons[0])
    vel = [cons[1] * inverse, cons[2] * inverse, cons[3] * inverse]
    pressure = (GAMMA - 1.0) * (
        cons[4] - 0.5 * (cons[1] * vel[0] + cons[2] * vel[1] + cons[3] * vel[2])
    )
    return inverse, vel, pressure


def shifted(me, step, count):
    moved = me + step
    return jnp.where(moved >= count, moved - count, moved)


def exchange_kernel(
    ngx, ngz, ny, state_ref, xpad, zt, alpha_ref, slots, mine, load_sem, send_sem, recv_sem,
    halo_send, halo_recv
):
    gx, gz = lax.axis_index("gx"), lax.axis_index("gz")
    rows = state_ref.shape[1]
    halo = 3 * ny
    load = pltpu.make_async_copy(state_ref, xpad.at[:, pl.ds(halo, rows), :], load_sem)
    load.start()
    barrier = pltpu.get_barrier_semaphore()
    offsets = [(dx, dz) for dx in range(ngx) for dz in range(ngz)][1:]
    peers = len(offsets)

    def each_peer(action):
        if peers < UNROLL_LIMIT:
            for slot, (dx, dz) in enumerate(offsets):
                action(slot, shifted(gx, dx, ngx), shifted(gz, dz, ngz))
        else:
            def body(slot, carry):
                dx, dz = (slot + 1) // ngz, (slot + 1) % ngz
                action(slot, shifted(gx, dx, ngx), shifted(gz, dz, ngz))
                return carry
            lax.fori_loop(0, peers, body, 0)

    def greet(slot, tx, tz):
        pl.semaphore_signal(barrier, inc=1, device_id=(tx, tz), device_id_type=MESH)

    each_peer(greet)
    load.wait()
    best = None
    for row in range(0, rows, 8):
        cons = [xpad[var, pl.ds(halo + row, 8), :] for var in range(5)]
        inverse, vel, pressure = pressure_velocity(cons)
        sound = jnp.sqrt(GAMMA * pressure * inverse)
        local = [jnp.abs(v) + sound for v in vel]
        best = local if best is None else [jnp.maximum(a, b) for a, b in zip(best, local)]
    tops = [jnp.max(jnp.max(b, axis=1, keepdims=True), axis=0, keepdims=True) for b in best]
    lane = lax.broadcasted_iota(jnp.int32, (1, 128), 1)
    mine[...] = jnp.where(lane == 0, tops[0], jnp.where(lane == 1, tops[1], tops[2]))
    for var in range(5):
        zt[var, pl.ds(8, 128), :] = xpad[var, pl.ds(halo, rows), :].T

    pl.semaphore_wait(barrier, peers)

    def send(slot, tx, tz):
        pltpu.make_async_remote_copy(
            src_ref=mine, dst_ref=slots.at[slot], send_sem=send_sem, recv_sem=recv_sem,
            device_id=(tx, tz), device_id_type=MESH,
        ).start()

    each_peer(send)
    right, left = shifted(gx, 1, ngx), shifted(gx, ngx - 1, ngx)
    high, low = shifted(gz, 1, ngz), shifted(gz, ngz - 1, ngz)
    moves = [
        (zt.at[:, pl.ds(8, 8), :], zt.at[:, pl.ds(136, 8), :], (gx, low)),
        (zt.at[:, pl.ds(128, 8), :], zt.at[:, pl.ds(0, 8), :], (gx, high)),
        (xpad.at[:, pl.ds(halo, halo), :], xpad.at[:, pl.ds(halo + rows, halo), :], (left, gz)),
        (xpad.at[:, pl.ds(rows, halo), :], xpad.at[:, pl.ds(0, halo), :], (right, gz)),
    ]
    copies = []
    for index, (src, dst, target) in enumerate(moves):
        copy = pltpu.make_async_remote_copy(
            src_ref=src, dst_ref=dst, send_sem=halo_send.at[index], recv_sem=halo_recv.at[index],
            device_id=target, device_id_type=MESH,
        )
        copy.start()
        copies.append(copy)
    pltpu.make_async_copy(slots, slots, recv_sem).wait()
    alpha_ref[...] = jnp.maximum(jnp.max(slots[...], axis=0), mine[...])
    for copy in copies:
        copy.wait()
    pltpu.make_async_copy(slots, slots, send_sem).wait()


class Line:
    def __init__(self, load):
        self.load = functools.lru_cache(None)(load)
        self.D = functools.lru_cache(None)(lambda j: self.load(j + 1) - self.load(j))
        self.S = functools.lru_cache(None)(lambda j: self.D(j) - self.D(j - 1))
        self.T = functools.lru_cache(None)(lambda j: self.S(j + 1) - self.S(j))
        self.S2 = functools.lru_cache(None)(lambda j: self.S(j) + self.S(j))
        self.C = functools.lru_cache(None)(
            lambda j: (self.S(j) * self.S(j) * (4.0 / 3.0) + 4.0 * EPS_WENO)
            + self.D(j) * self.D(j - 1)
        )

    def L(self, j):
        return self.C(j) + self.S2(j) * self.D(j)

    def R(self, j):
        return self.C(j) - self.S2(j) * self.D(j - 1)


def correction(near, mid, far, t_near, t_far):
    a, b, c = mid * far, near * far, near * mid
    w_near = a * a
    w_far = 3.0 * (c * c)
    total = w_near + 6.0 * (b * b) + w_far
    return (w_far * t_far + (w_near + w_near) * t_near) * reciprocal(total)


def line_divergence(count, load_plus, load_minus, emit):
    plus, minus = Line(load_plus), Line(load_minus)
    twice = functools.lru_cache(None)(lambda j: plus.load(j) + minus.load(j))

    def face(j):
        up = correction(plus.L(j - 1), plus.C(j), plus.R(j + 1), plus.T(j - 1), plus.T(j))
        down = correction(minus.R(j + 2), minus.C(j + 1), minus.L(j), minus.T(j + 1), minus.T(j))
        return (
            3.0 * (twice(j) + twice(j + 1)) - (plus.S(j) + minus.S(j + 1)) - up + down
        )

    before = face(2)
    for cell in range(count):
        j = cell + 3
        after = face(j)
        central = (
            4.5 * (twice(j + 1) - twice(j - 1))
            - 0.9 * (twice(j + 2) - twice(j - 2))
            + 0.1 * (twice(j + 3) - twice(j - 3))
        )
        emit(cell, after - before, central)
        before = after


def split_fluxes(cons, var, alpha, fp, fm, cell):
    _, vel, pressure = pressure_velocity(cons)
    velocity = vel[var - 1]
    for field in range(5):
        if field == 4:
            flux = (cons[4] + pressure) * velocity
        else:
            flux = cons[field] * velocity
        if field == var:
            flux = flux + pressure
        drift = alpha * cons[field]
        fp[field, cell] = flux + drift
        fm[field, cell] = flux - drift


def update_kernel(
    cx, ny, xpad, zt, alpha_ref, register, top_ghost, flags, new_state, new_register,
    mask, mask_t, acc, acc_t, fp, fm
):
    halo = 3 * ny
    rows = cx * ny
    strip = zt.shape[1] - 16
    chunk = strip // 8
    alpha = [jnp.broadcast_to(alpha_ref[:, k : k + 1], (8, 128)) for k in range(3)]
    mask[...] = jnp.broadcast_to(flags[...], (rows, 128)).astype(jnp.float32)
    mask_t[...] = mask[...].T[:8]

    for cell in range(chunk + 6):
        cons = [zt[f, pl.ds(5 + cell, 8, stride=chunk), :] for f in range(5)]
        split_fluxes(cons, 3, alpha[2], fp, fm, cell)
    flag_t = mask_t[...] > 0.0

    def z_field(f, carry):
        def emit(cell, upwind, central):
            acc_t[f, pl.ds(cell, 8, stride=chunk), :] = (LAMBDA[2] / 12.0) * jnp.where(
                flag_t, upwind, central
            )
        line_divergence(chunk, lambda j: fp[f, j], lambda j: fm[f, j], emit)
        return carry

    lax.fori_loop(0, 5, z_field, 0)

    for part in range(0, ny, 8):
        for cell in range(cx + 6):
            cons = [xpad[f, pl.ds(cell * ny + part, 8), :] for f in range(5)]
            split_fluxes(cons, 1, alpha[0], fp, fm, cell)

        def x_field(f, carry):
            def emit(cell, upwind, central):
                where = pl.ds(cell * ny + part, 8)
                acc[f, where, :] = (LAMBDA[0] / 12.0) * jnp.where(
                    mask[where, :] > 0.0, upwind, central
                )
            line_divergence(cx, lambda j: fp[f, j], lambda j: fm[f, j], emit)
            return carry

        lax.fori_loop(0, 5, x_field, 0)

    for cell in range(ny + 6):
        y = cell - 3
        if y < ny:
            source = y if y >= 0 else -1 - y
            cons = [xpad[f, pl.ds(halo + source, 8, stride=ny), :] for f in range(5)]
            if y < 0:
                cons[2] = -cons[2]
        else:
            cons = [top_ghost[f, :, y - ny, :] for f in range(5)]
        split_fluxes(cons, 2, alpha[1], fp, fm, cell)

    def y_field(f, carry):
        def emit(cell, upwind, central):
            where = pl.ds(cell, 8, stride=ny)
            acc[f, where, :] = acc[f, where, :] + (LAMBDA[1] / 12.0) * jnp.where(
                mask[where, :] > 0.0, upwind, central
            )
        line_divergence(ny, lambda j: fp[f, j], lambda j: fm[f, j], emit)
        return carry

    lax.fori_loop(0, 5, y_field, 0)

    for f in range(5):
        total = acc[f] + acc_t[f].T
        updated = REGISTER_DECAY * register[f] - total
        new_register[f] = updated
        new_state[f] = xpad[f, pl.ds(halo, rows), :] + UPDATE_WEIGHT * updated


def shards(ngx, ngz, state, register, top_ghost, flags):
    _, cx, ny, cz = state.shape
    rows = cx * ny
    vmem = pl.BlockSpec(memory_space=pltpu.VMEM)
    flat = state.reshape(5, rows, cz)
    peers = ngx * ngz - 1
    f32 = jnp.float32
    xpad, zt, alpha = pl.pallas_call(
        functools.partial(exchange_kernel, ngx, ngz, ny),
        out_shape=(
            jax.ShapeDtypeStruct((5, (cx + 6) * ny, cz), f32),
            jax.ShapeDtypeStruct((5, cz + 16, rows), f32),
            jax.ShapeDtypeStruct((1, 128), f32),
        ),
        in_specs=[pl.BlockSpec(memory_space=pl.ANY)],
        out_specs=[vmem] * 3,
        scratch_shapes=[
            pltpu.VMEM((peers, 1, 128), f32),
            pltpu.VMEM((1, 128), f32),
            pltpu.SemaphoreType.DMA,
            pltpu.SemaphoreType.DMA,
            pltpu.SemaphoreType.DMA,
            pltpu.SemaphoreType.DMA((4,)),
            pltpu.SemaphoreType.DMA((4,)),
        ],
        compiler_params=pltpu.CompilerParams(collective_id=0, has_side_effects=True),
        name="exchange",
    )(flat)
    longest = max(cx, ny, cz // 8) + 6
    new_state, new_register = pl.pallas_call(
        functools.partial(update_kernel, cx, ny),
        out_shape=(jax.ShapeDtypeStruct((5, rows, cz), f32),) * 2,
        in_specs=[vmem] * 6,
        out_specs=[vmem] * 2,
        scratch_shapes=[
            pltpu.VMEM((rows, 128), f32),
            pltpu.VMEM((8, 128), f32),
            pltpu.VMEM((5, rows, cz), f32),
            pltpu.VMEM((5, cz, rows), f32),
            pltpu.VMEM((5, longest, 8, 128), f32),
            pltpu.VMEM((5, longest, 8, 128), f32),
        ],
        name="update",
    )(xpad, zt, alpha, register.reshape(5, rows, cz), top_ghost, flags.reshape(rows, 1))
    return new_state.reshape(state.shape), new_register.reshape(state.shape)


def solution(mesh):
    block = P(None, "gx", None, "gz")
    return jax.shard_map(
        functools.partial(shards, mesh.shape["gx"], mesh.shape["gz"]),
        mesh=mesh,
        in_specs=(block, block, block, P("gx", None, "gz")),
        out_specs=(block, block),
        check_vma=False,
    )
```

```python
import functools

import jax
import jax.numpy as jnp
from jax import lax
from jax.experimental import pallas as pl
from jax.experimental.pallas import tpu as pltpu
from jax.sharding import PartitionSpec as P

MESH = pl.DeviceIdType.MESH
GAMMA = 1.4
EPS_WENO = 1e-06
LAMBDA = (0.1, 0.15, 0.1)
REGISTER_DECAY = -5.0 / 9.0
UPDATE_WEIGHT = 15.0 / 16.0
UNROLL_LIMIT = 64


def reciprocal(value):
    guess = pl.reciprocal(value, approx=True)
    return guess * (2.0 - value * guess)


def pressure_velocity(cons):
    inverse = reciprocal(cons[0])
    vel = [cons[1] * inverse, cons[2] * inverse, cons[3] * inverse]
    pressure = (GAMMA - 1.0) * (
        cons[4] - 0.5 * (cons[1] * vel[0] + cons[2] * vel[1] + cons[3] * vel[2])
    )
    return inverse, vel, pressure


def shifted(me, step, count):
    moved = me + step
    return jnp.where(moved >= count, moved - count, moved)


def exchange_peers(gx, gz, ngx, ngz):
    offsets = [(dx, dz) for dx in range(ngx) for dz in range(ngz)][1:]

    def each_peer(action):
        if len(offsets) < UNROLL_LIMIT:
            for slot, (dx, dz) in enumerate(offsets):
                action(slot, shifted(gx, dx, ngx), shifted(gz, dz, ngz))
        else:
            def body(slot, carry):
                dx, dz = (slot + 1) // ngz, (slot + 1) % ngz
                action(slot, shifted(gx, dx, ngx), shifted(gz, dz, ngz))
                return carry
            lax.fori_loop(0, len(offsets), body, 0)

    return each_peer, len(offsets)


class Line:
    def __init__(self, load):
        cached = functools.lru_cache(None)
        self.load = cached(load)
        self.D = cached(lambda j: self.load(j + 1) - self.load(j))
        self.S = cached(lambda j: self.D(j) - self.D(j - 1))
        self.T = cached(lambda j: self.S(j + 1) - self.S(j))
        self.S2 = cached(lambda j: self.S(j) + self.S(j))
        self.C = cached(
            lambda j: (self.S(j) * self.S(j) * (4.0 / 3.0) + 4.0 * EPS_WENO)
            + self.D(j) * self.D(j - 1)
        )

    def L(self, j):
        return self.C(j) + self.S2(j) * self.D(j)

    def R(self, j):
        return self.C(j) - self.S2(j) * self.D(j - 1)


def correction(near, mid, far, t_near, t_far):
    a, b, c = mid * far, near * far, near * mid
    w_near = a * a
    w_far = 3.0 * (c * c)
    total = w_near + 6.0 * (b * b) + w_far
    return (w_far * t_far + (w_near + w_near) * t_near) * reciprocal(total)


def line_divergence(count, alpha, load_flux, load_cons, emit):
    flux = functools.lru_cache(None)(load_flux)
    drift = functools.lru_cache(None)(lambda j: alpha * load_cons(j))
    plus, minus = Line(lambda j: flux(j) + drift(j)), Line(lambda j: flux(j) - drift(j))

    def face(j):
        up = correction(plus.L(j - 1), plus.C(j), plus.R(j + 1), plus.T(j - 1), plus.T(j))
        down = correction(minus.R(j + 2), minus.C(j + 1), minus.L(j), minus.T(j + 1), minus.T(j))
        return 6.0 * (flux(j) + flux(j + 1)) - (plus.S(j) + minus.S(j + 1)) - up + down

    before = face(2)
    for cell in range(count):
        j = cell + 3
        after = face(j)
        central = (
            9.0 * (flux(j + 1) - flux(j - 1))
            - 1.8 * (flux(j + 2) - flux(j - 2))
            + 0.2 * (flux(j + 3) - flux(j - 3))
        )
        emit(cell, after - before, central)
        before = after


def store_fluxes(cons, var, fluxes, conserved, cell):
    _, vel, pressure = pressure_velocity(cons)
    velocity = vel[var - 1]
    for field in range(5):
        if field == 4:
            flux = (cons[4] + pressure) * velocity
        else:
            flux = cons[field] * velocity
        if field == var:
            flux = flux + pressure
        fluxes[field, cell] = flux
        conserved[field, cell] = cons[field]


def step_kernel(
    ngx, ngz, cx, ny, state_ref, ghost_ref, flags_ref, change_ref, xpad, zt, ghost, flags,
    slots, mine, mask, acc, acc_t, zf, zu, yf, yu, xf, xu,
    load_sem, side_sem, send_sem, recv_sem, halo_send, halo_recv, out_sem
):
    gx, gz = lax.axis_index("gx"), lax.axis_index("gz")
    rows = cx * ny
    halo = 3 * ny
    strip = zt.shape[1] - 16
    chunk = strip // 8
    load = pltpu.make_async_copy(state_ref, xpad.at[:, pl.ds(halo, rows), :], load_sem)
    load.start()
    load_flags = pltpu.make_async_copy(flags_ref, flags, side_sem.at[0])
    load_flags.start()
    load_ghost = pltpu.make_async_copy(ghost_ref, ghost, side_sem.at[1])
    load_ghost.start()
    barrier = pltpu.get_barrier_semaphore()
    each_peer, peers = exchange_peers(gx, gz, ngx, ngz)

    def greet(slot, tx, tz):
        pl.semaphore_signal(barrier, inc=1, device_id=(tx, tz), device_id_type=MESH)

    each_peer(greet)
    load.wait()
    best = None
    for row in range(0, rows, 8):
        cons = [xpad[var, pl.ds(halo + row, 8), :] for var in range(5)]
        inverse, vel, pressure = pressure_velocity(cons)
        sound = jnp.sqrt(GAMMA * pressure * inverse)
        local = [jnp.abs(v) + sound for v in vel]
        best = local if best is None else [jnp.maximum(a, b) for a, b in zip(best, local)]
    tops = [jnp.max(jnp.max(b, axis=0, keepdims=True), axis=1, keepdims=True) for b in best]
    lane = lax.broadcasted_iota(jnp.int32, (1, 128), 1)
    mine[...] = jnp.where(lane == 0, tops[0], jnp.where(lane == 1, tops[1], tops[2]))

    pl.semaphore_wait(barrier, peers)

    def send(slot, tx, tz):
        pltpu.make_async_remote_copy(
            src_ref=mine, dst_ref=slots.at[slot], send_sem=send_sem, recv_sem=recv_sem,
            device_id=(tx, tz), device_id_type=MESH,
        ).start()

    each_peer(send)
    right, left = shifted(gx, 1, ngx), shifted(gx, ngx - 1, ngx)
    high, low = shifted(gz, 1, ngz), shifted(gz, ngz - 1, ngz)

    def move(index, src, dst, target):
        copy = pltpu.make_async_remote_copy(
            src_ref=src, dst_ref=dst, send_sem=halo_send.at[index], recv_sem=halo_recv.at[index],
            device_id=target, device_id_type=MESH,
        )
        copy.start()
        return copy

    x_copies = [
        move(0, xpad.at[:, pl.ds(halo, halo), :], xpad.at[:, pl.ds(halo + rows, halo), :], (left, gz)),
        move(1, xpad.at[:, pl.ds(rows, halo), :], xpad.at[:, pl.ds(0, halo), :], (right, gz)),
    ]
    for var in range(5):
        zt[var, pl.ds(8, strip), :] = xpad[var, pl.ds(halo, rows), :].T
    load_flags.wait()
    for x in range(cx):
        wide = jnp.broadcast_to(flags[x], (strip, ny)).astype(jnp.float32)
        mask[pl.ds(x * ny, ny), :] = wide.T
    z_copies = [
        move(2, zt.at[:, pl.ds(8, 8), :], zt.at[:, pl.ds(8 + strip, 8), :], (gx, low)),
        move(3, zt.at[:, pl.ds(strip, 8), :], zt.at[:, pl.ds(0, 8), :], (gx, high)),
    ]
    flag_t = mask[...].T[:8] > 0.0

    load_ghost.wait()
    for cell in range(ny + 6):
        y = cell - 3
        if y < ny:
            source = y if y >= 0 else -1 - y
            cons = [xpad[f, pl.ds(halo + source, 8, stride=ny), :] for f in range(5)]
            if y < 0:
                cons[2] = -cons[2]
        else:
            cons = [ghost[f, y - ny] for f in range(5)]
        store_fluxes(cons, 2, yf, yu, cell)

    for copy in z_copies:
        copy.wait()
    for cell in range(chunk + 6):
        cons = [zt[f, pl.ds(5 + cell, 8, stride=chunk), :] for f in range(5)]
        store_fluxes(cons, 3, zf, zu, cell)

    pltpu.make_async_copy(slots, slots, recv_sem).wait()
    top = jnp.maximum(jnp.max(slots[...], axis=0), mine[...])
    alpha = [jnp.broadcast_to(top[:, k : k + 1], (8, 128)) for k in range(3)]

    def z_field(f, carry):
        def emit(cell, upwind, central):
            acc_t[f, pl.ds(cell, 8, stride=chunk), :] = (LAMBDA[2] / 12.0) * jnp.where(
                flag_t, upwind, central
            )
        line_divergence(chunk, alpha[2], lambda j: zf[f, j], lambda j: zu[f, j], emit)
        return carry

    lax.fori_loop(0, 5, z_field, 0)
    for f in range(5):
        acc[f] = acc_t[f].T

    def y_field(f, carry):
        def emit(cell, upwind, central):
            where = pl.ds(cell, 8, stride=ny)
            acc[f, where, :] = acc[f, where, :] + (LAMBDA[1] / 12.0) * jnp.where(
                mask[where, :] > 0.0, upwind, central
            )
        line_divergence(ny, alpha[1], lambda j: yf[f, j], lambda j: yu[f, j], emit)
        return carry

    lax.fori_loop(0, 5, y_field, 0)

    for copy in x_copies:
        copy.wait()
    for part in range(ny // 8):
        for cell in range(cx + 6):
            cons = [xpad[f, pl.ds(cell * ny + part * 8, 8), :] for f in range(5)]
            store_fluxes(cons, 1, xf.at[part], xu.at[part], cell)

    def x_field(f, carry):
        for part in range(ny // 8):
            def emit(cell, upwind, central):
                where = pl.ds(cell * ny + part * 8, 8)
                acc[f, where, :] = acc[f, where, :] + (LAMBDA[0] / 12.0) * jnp.where(
                    mask[where, :] > 0.0, upwind, central
                )
            line_divergence(
                cx, alpha[0], lambda j: xf[part, f, j], lambda j: xu[part, f, j], emit
            )
        pltpu.make_async_copy(acc.at[f], change_ref.at[f], out_sem).start()
        return carry

    lax.fori_loop(0, 5, x_field, 0)
    pltpu.make_async_copy(slots, slots, send_sem).wait()
    pltpu.make_async_copy(acc, change_ref, out_sem).wait()


def shards(ngx, ngz, state, register, top_ghost, flags):
    _, cx, ny, cz = state.shape
    rows = cx * ny
    peers = ngx * ngz - 1
    f32 = jnp.float32
    anywhere = pl.BlockSpec(memory_space=pl.ANY)
    flat = state.reshape(5, rows, cz)
    change = pl.pallas_call(
        functools.partial(step_kernel, ngx, ngz, cx, ny),
        out_shape=jax.ShapeDtypeStruct((5, rows, cz), f32),
        in_specs=[anywhere] * 3,
        out_specs=anywhere,
        scratch_shapes=[
            pltpu.VMEM((5, (cx + 6) * ny, cz), f32),
            pltpu.VMEM((5, cz + 16, rows), f32),
            pltpu.VMEM((5, 3, cx, cz), f32),
            pltpu.VMEM((cx, 1, ny), jnp.int32),
            pltpu.VMEM((peers, 1, 128), f32),
            pltpu.VMEM((1, 128), f32),
            pltpu.VMEM((rows, cz), f32),
            pltpu.VMEM((5, rows, cz), f32),
            pltpu.VMEM((5, cz, rows), f32),
            pltpu.VMEM((5, cz // 8 + 6, 8, rows), f32),
            pltpu.VMEM((5, cz // 8 + 6, 8, rows), f32),
            pltpu.VMEM((5, ny + 6, 8, cz), f32),
            pltpu.VMEM((5, ny + 6, 8, cz), f32),
            pltpu.VMEM((ny // 8, 5, cx + 6, 8, cz), f32),
            pltpu.VMEM((ny // 8, 5, cx + 6, 8, cz), f32),
            pltpu.SemaphoreType.DMA,
            pltpu.SemaphoreType.DMA((2,)),
            pltpu.SemaphoreType.DMA,
            pltpu.SemaphoreType.DMA,
            pltpu.SemaphoreType.DMA((4,)),
            pltpu.SemaphoreType.DMA((4,)),
            pltpu.SemaphoreType.DMA,
        ],
        compiler_params=pltpu.CompilerParams(collective_id=0, has_side_effects=True),
        name="step",
    )(flat, top_ghost.transpose(0, 2, 1, 3), flags.transpose(0, 2, 1))
    new_register = REGISTER_DECAY * register - change.reshape(state.shape)
    new_state = state + UPDATE_WEIGHT * new_register
    return new_state, new_register


def solution(mesh):
    block = P(None, "gx", None, "gz")
    return jax.shard_map(
        functools.partial(shards, mesh.shape["gx"], mesh.shape["gz"]),
        mesh=mesh,
        in_specs=(block, block, block, P("gx", None, "gz")),
        out_specs=(block, block),
        check_vma=False,
    )
```

```python
import functools

import jax
import jax.numpy as jnp
from jax import lax
from jax.experimental import pallas as pl
from jax.experimental.pallas import tpu as pltpu
from jax.sharding import PartitionSpec as P

MESH = pl.DeviceIdType.MESH
GAMMA = 1.4
EPS_WENO = 1e-06
LAMBDA = (0.1, 0.15, 0.1)
REGISTER_DECAY = -5.0 / 9.0
UPDATE_WEIGHT = 15.0 / 16.0
UNROLL_LIMIT = 64


def reciprocal(value):
    guess = pl.reciprocal(value, approx=True)
    return guess * (2.0 - value * guess)


def pressure_velocity(cons):
    inverse = reciprocal(cons[0])
    vel = [cons[1] * inverse, cons[2] * inverse, cons[3] * inverse]
    pressure = (GAMMA - 1.0) * (
        cons[4] - 0.5 * (cons[1] * vel[0] + cons[2] * vel[1] + cons[3] * vel[2])
    )
    return inverse, vel, pressure


def shifted(me, step, count):
    moved = me + step
    return jnp.where(moved >= count, moved - count, moved)


def exchange_peers(gx, gz, ngx, ngz):
    offsets = [(dx, dz) for dx in range(ngx) for dz in range(ngz)][1:]

    def each_peer(action):
        if len(offsets) < UNROLL_LIMIT:
            for slot, (dx, dz) in enumerate(offsets):
                action(slot, shifted(gx, dx, ngx), shifted(gz, dz, ngz))
        else:
            def body(slot, carry):
                dx, dz = (slot + 1) // ngz, (slot + 1) % ngz
                action(slot, shifted(gx, dx, ngx), shifted(gz, dz, ngz))
                return carry
            lax.fori_loop(0, len(offsets), body, 0)

    return each_peer, len(offsets)


class Line:
    def __init__(self, load):
        cached = functools.lru_cache(None)
        self.load = cached(load)
        self.D = cached(lambda j: self.load(j + 1) - self.load(j))
        self.S = cached(lambda j: self.D(j) - self.D(j - 1))
        self.T = cached(lambda j: self.S(j + 1) - self.S(j))
        self.S2 = cached(lambda j: self.S(j) + self.S(j))
        self.C = cached(
            lambda j: (self.S(j) * self.S(j) * (4.0 / 3.0) + 4.0 * EPS_WENO)
            + self.D(j) * self.D(j - 1)
        )

    def L(self, j):
        return self.C(j) + self.S2(j) * self.D(j)

    def R(self, j):
        return self.C(j) - self.S2(j) * self.D(j - 1)


def correction(near, mid, far, t_near, t_far):
    a, b, c = mid * far, near * far, near * mid
    w_near = a * a
    w_far = 3.0 * (c * c)
    total = w_near + 6.0 * (b * b) + w_far
    return (w_far * t_far + (w_near + w_near) * t_near) * reciprocal(total)


def line_divergence(count, alpha, load_flux, load_cons, emit):
    flux = functools.lru_cache(None)(load_flux)
    drift = functools.lru_cache(None)(lambda j: alpha * load_cons(j))
    plus, minus = Line(lambda j: flux(j) + drift(j)), Line(lambda j: flux(j) - drift(j))

    def face(j):
        up = correction(plus.L(j - 1), plus.C(j), plus.R(j + 1), plus.T(j - 1), plus.T(j))
        down = correction(minus.R(j + 2), minus.C(j + 1), minus.L(j), minus.T(j + 1), minus.T(j))
        return 6.0 * (flux(j) + flux(j + 1)) - (plus.S(j) + minus.S(j + 1)) - up + down

    before = face(2)
    for cell in range(count):
        j = cell + 3
        after = face(j)
        central = (
            9.0 * (flux(j + 1) - flux(j - 1))
            - 1.8 * (flux(j + 2) - flux(j - 2))
            + 0.2 * (flux(j + 3) - flux(j - 3))
        )
        emit(cell, after - before, central)
        before = after


def store_fluxes(cons, var, fluxes, conserved, cell):
    _, vel, pressure = pressure_velocity(cons)
    velocity = vel[var - 1]
    for field in range(5):
        if field == 4:
            flux = (cons[4] + pressure) * velocity
        else:
            flux = cons[field] * velocity
        if field == var:
            flux = flux + pressure
        fluxes[field, cell] = flux
        conserved[field, cell] = cons[field]


def step_kernel(
    ngx, ngz, cx, ny, state_ref, ghost_ref, flags_ref, acc, xpad, zt, ghost, flags,
    slots, mine, mask, acc_t, zf, zu, yf, yu, xf, xu,
    load_sem, side_sem, send_sem, recv_sem, halo_send, halo_recv, out_sem
):
    gx, gz = lax.axis_index("gx"), lax.axis_index("gz")
    rows = cx * ny
    halo = 3 * ny
    strip = zt.shape[1] - 16
    chunk = strip // 8
    load = pltpu.make_async_copy(state_ref, xpad.at[:, pl.ds(halo, rows), :], load_sem)
    load.start()
    load_flags = pltpu.make_async_copy(flags_ref, flags, side_sem.at[0])
    load_flags.start()
    load_ghost = pltpu.make_async_copy(ghost_ref, ghost, side_sem.at[1])
    load_ghost.start()
    barrier = pltpu.get_barrier_semaphore()
    each_peer, peers = exchange_peers(gx, gz, ngx, ngz)

    def greet(slot, tx, tz):
        pl.semaphore_signal(barrier, inc=1, device_id=(tx, tz), device_id_type=MESH)

    each_peer(greet)
    load.wait()
    best = None
    for row in range(0, rows, 8):
        cons = [xpad[var, pl.ds(halo + row, 8), :] for var in range(5)]
        inverse, vel, pressure = pressure_velocity(cons)
        sound = jnp.sqrt(GAMMA * pressure * inverse)
        local = [jnp.abs(v) + sound for v in vel]
        best = local if best is None else [jnp.maximum(a, b) for a, b in zip(best, local)]
    tops = [jnp.max(jnp.max(b, axis=0, keepdims=True), axis=1, keepdims=True) for b in best]
    lane = lax.broadcasted_iota(jnp.int32, (1, 128), 1)
    mine[...] = jnp.where(lane == 0, tops[0], jnp.where(lane == 1, tops[1], tops[2]))

    pl.semaphore_wait(barrier, peers)

    def send(slot, tx, tz):
        pltpu.make_async_remote_copy(
            src_ref=mine, dst_ref=slots.at[slot], send_sem=send_sem, recv_sem=recv_sem,
            device_id=(tx, tz), device_id_type=MESH,
        ).start()

    each_peer(send)
    right, left = shifted(gx, 1, ngx), shifted(gx, ngx - 1, ngx)
    high, low = shifted(gz, 1, ngz), shifted(gz, ngz - 1, ngz)

    def move(index, src, dst, target):
        copy = pltpu.make_async_remote_copy(
            src_ref=src, dst_ref=dst, send_sem=halo_send.at[index], recv_sem=halo_recv.at[index],
            device_id=target, device_id_type=MESH,
        )
        copy.start()
        return copy

    x_copies = [
        move(0, xpad.at[:, pl.ds(halo, halo), :], xpad.at[:, pl.ds(halo + rows, halo), :], (left, gz)),
        move(1, xpad.at[:, pl.ds(rows, halo), :], xpad.at[:, pl.ds(0, halo), :], (right, gz)),
    ]
    for var in range(5):
        zt[var, pl.ds(8, strip), :] = xpad[var, pl.ds(halo, rows), :].T
    load_flags.wait()
    for x in range(cx):
        wide = jnp.broadcast_to(flags[x], (strip, ny)).astype(jnp.float32)
        mask[pl.ds(x * ny, ny), :] = wide.T
    z_copies = [
        move(2, zt.at[:, pl.ds(8, 8), :], zt.at[:, pl.ds(8 + strip, 8), :], (gx, low)),
        move(3, zt.at[:, pl.ds(strip, 8), :], zt.at[:, pl.ds(0, 8), :], (gx, high)),
    ]
    flag_t = mask[...].T[:8] > 0.0

    load_ghost.wait()
    for cell in range(ny + 6):
        y = cell - 3
        if y < ny:
            source = y if y >= 0 else -1 - y
            cons = [xpad[f, pl.ds(halo + source, 8, stride=ny), :] for f in range(5)]
            if y < 0:
                cons[2] = -cons[2]
        else:
            cons = [ghost[f, y - ny] for f in range(5)]
        store_fluxes(cons, 2, yf, yu, cell)

    for copy in z_copies:
        copy.wait()
    for cell in range(chunk + 6):
        cons = [zt[f, pl.ds(5 + cell, 8, stride=chunk), :] for f in range(5)]
        store_fluxes(cons, 3, zf, zu, cell)

    pltpu.make_async_copy(slots, slots, recv_sem).wait()
    top = jnp.maximum(jnp.max(slots[...], axis=0), mine[...])
    alpha = [jnp.broadcast_to(top[:, k : k + 1], (8, 128)) for k in range(3)]

    def z_field(f, carry):
        def emit(cell, upwind, central):
            acc_t[f, pl.ds(cell, 8, stride=chunk), :] = (LAMBDA[2] / 12.0) * jnp.where(
                flag_t, upwind, central
            )
        line_divergence(chunk, alpha[2], lambda j: zf[f, j], lambda j: zu[f, j], emit)
        return carry

    lax.fori_loop(0, 5, z_field, 0)
    for f in range(5):
        acc[f] = acc_t[f].T

    def y_field(f, carry):
        def emit(cell, upwind, central):
            where = pl.ds(cell, 8, stride=ny)
            acc[f, where, :] = acc[f, where, :] + (LAMBDA[1] / 12.0) * jnp.where(
                mask[where, :] > 0.0, upwind, central
            )
        line_divergence(ny, alpha[1], lambda j: yf[f, j], lambda j: yu[f, j], emit)
        return carry

    lax.fori_loop(0, 5, y_field, 0)

    for copy in x_copies:
        copy.wait()
    for part in range(ny // 8):
        for cell in range(cx + 6):
            cons = [xpad[f, pl.ds(cell * ny + part * 8, 8), :] for f in range(5)]
            store_fluxes(cons, 1, xf.at[part], xu.at[part], cell)

    def x_field(f, carry):
        for part in range(ny // 8):
            def emit(cell, upwind, central):
                where = pl.ds(cell * ny + part * 8, 8)
                acc[f, where, :] = acc[f, where, :] + (LAMBDA[0] / 12.0) * jnp.where(
                    mask[where, :] > 0.0, upwind, central
                )
            line_divergence(
                cx, alpha[0], lambda j: xf[part, f, j], lambda j: xu[part, f, j], emit
            )
        return carry

    lax.fori_loop(0, 5, x_field, 0)
    pltpu.make_async_copy(slots, slots, send_sem).wait()


def shards(ngx, ngz, state, register, top_ghost, flags):
    _, cx, ny, cz = state.shape
    rows = cx * ny
    peers = ngx * ngz - 1
    f32 = jnp.float32
    anywhere = pl.BlockSpec(memory_space=pl.ANY)
    flat = state.reshape(5, rows, cz)
    change = pl.pallas_call(
        functools.partial(step_kernel, ngx, ngz, cx, ny),
        out_shape=pltpu.VMEM((5, rows, cz), f32),
        in_specs=[anywhere] * 3,
        out_specs=pl.BlockSpec(memory_space=pltpu.VMEM),
        scratch_shapes=[
            pltpu.VMEM((5, (cx + 6) * ny, cz), f32),
            pltpu.VMEM((5, cz + 16, rows), f32),
            pltpu.VMEM((5, 3, cx, cz), f32),
            pltpu.VMEM((cx, 1, ny), jnp.int32),
            pltpu.VMEM((peers, 1, 128), f32),
            pltpu.VMEM((1, 128), f32),
            pltpu.VMEM((rows, cz), f32),
            pltpu.VMEM((5, cz, rows), f32),
            pltpu.VMEM((5, cz // 8 + 6, 8, rows), f32),
            pltpu.VMEM((5, cz // 8 + 6, 8, rows), f32),
            pltpu.VMEM((5, ny + 6, 8, cz), f32),
            pltpu.VMEM((5, ny + 6, 8, cz), f32),
            pltpu.VMEM((ny // 8, 5, cx + 6, 8, cz), f32),
            pltpu.VMEM((ny // 8, 5, cx + 6, 8, cz), f32),
            pltpu.SemaphoreType.DMA,
            pltpu.SemaphoreType.DMA((2,)),
            pltpu.SemaphoreType.DMA,
            pltpu.SemaphoreType.DMA,
            pltpu.SemaphoreType.DMA((4,)),
            pltpu.SemaphoreType.DMA((4,)),
            pltpu.SemaphoreType.DMA,
        ],
        compiler_params=pltpu.CompilerParams(collective_id=0, has_side_effects=True),
        name="step",
    )(flat, top_ghost.transpose(0, 2, 1, 3), flags.transpose(0, 2, 1))
    new_register = REGISTER_DECAY * register - change.reshape(state.shape)
    new_state = state + UPDATE_WEIGHT * new_register
    return new_state, new_register


def solution(mesh):
    block = P(None, "gx", None, "gz")
    return jax.shard_map(
        functools.partial(shards, mesh.shape["gx"], mesh.shape["gz"]),
        mesh=mesh,
        in_specs=(block, block, block, P("gx", None, "gz")),
        out_specs=(block, block),
        check_vma=False,
    )
```
